512 devices in a mesh: group: 2 (over y), expert: 64 (over z, core), tensor: 4 (over x).
Axes of the slice: x: 4, y: 2, z: 32, core: 2. Of those that a mesh axis runs over, the one named last changes fastest.
The devices are a block of a 4x8x32 slice.
Arguments:
- tokens: bfloat16 [4096, 4096], P(('group', 'expert'), 'tensor'), parts along dimension 0, may hold values from -6 to 6
- expert_ids: int32 [4096, 8], P(('group', 'expert')), parts along dimension 0, may hold values from 0 to 63, all different within a row; in each aligned block of 32 rows (0 to 31, 32 to 63, ...) at most 6 rows name the same one
- router_logits: float32 [4096, 8], P(('group', 'expert')), parts along dimension 0, may hold values from -6 to 6
- up_weight: bfloat16 [64, 4096, 1024], P('expert', None, 'tensor'), may hold values from -0.09375 to 0.09375
- down_weight: bfloat16 [64, 1024, 4096], P('expert', 'tensor'), may hold values from -0.1875 to 0.1875
Outputs:
- moe_out: bfloat16 [4096, 4096], P(('group', 'expert'), 'tensor'), parts along dimension 0
The draws below stay inside these ranges and needn't reach their ends.
There are 2 independent parts, one for each index of `group`. The reference program is written for one: setup_inputs(seed, part) draws one part's arguments, and reference() takes and returns one part's arrays. A program takes and returns all parts, laid end to end along the dimension named above; an argument that names none is the same for every part. Nothing has to cross between parts.
Inputs may be any that keep to these rules, and one draw needn't show every extreme that they name: `expert_ids`: each row names 8 different experts. In each aligned block of 32 rows (the rows of one index of the expert axis) no expert is named by more than 6 rows, a bound that some block reaches.
All inputs are finite; a program needn't handle non-finite values.
Results may differ from the reference program's by a relative error of at most 0.014.
Values may be sent and summed in bfloat16 or wider, within the bound.
No kernel may reach another device: no remote copies, remote signals or barrier semaphores. Data moves between devices by JAX's collectives and lax.ppermute only.
A program may use at most 64 MiB of HBM per device.

```python
import math
import jax
import jax.numpy as jnp
import numpy as np
from jax import lax

TOK_DEV = 32
D = 4096
FF = 1024
EXPERTS = 64
TOP = 8
CAP = 6
TOKENS = 2048
N_EXPERT = 64
N_TENSOR = 4


def block_scale(own_key, dims, split, low, top_value):
    def one(position, shards_of):
        heights = jax.random.uniform(jax.random.fold_in(jax.random.fold_in(own_key, 6), position), (shards_of,), jnp.float32, low / len(split), top_value / len(split))
        return jnp.repeat(jnp.exp(heights), dims[position] // shards_of).reshape((-1,) + (1,) * (len(dims) - position - 1))

    loudness = one(*split[0])
    for cut in split[1:]:
        loudness = loudness * one(*cut)
    return loudness


def deal_out(rng, own, number, rows, number_of, top, most, slope):
    ranking = jax.random.permutation(rng, number_of)
    crowded, ordinary = load_shares(number_of, rows * top, most, slope, True), load_shares(number_of, rows * top, most, slope, False)
    places = jnp.arange(number_of)

    def named(tallies, turn):
        used = int((tallies > 0).sum())
        fixed = max(1, used // 4)
        passed = fixed + (places - fixed + turn * (used - fixed)) % max(1, number_of - fixed)
        return jnp.zeros((number_of,), jnp.int32).at[ranking[jnp.where(places < fixed, places, passed)]].set(jnp.asarray(tallies, jnp.int32))

    tallies = jnp.where(number % 4 == 0, named(crowded, number // 4), named(ordinary, number - number // 4 - 1))
    mixed = jax.random.permutation(jax.random.fold_in(own, 3), number_of)
    source_of, sink = mixed[0:number_of // 2 * 2:2], mixed[1:number_of // 2 * 2:2]
    margin = jnp.minimum(tallies[source_of] - 1, most - tallies[sink]) // 2
    margin = jnp.where((source_of == ranking[0]) | (sink == ranking[0]) | (tallies[sink] == 0), 0, jnp.maximum(margin, 0))
    passed = jax.random.randint(jax.random.fold_in(own, 4), (number_of // 2,), 0, 1 << 20) % (margin + 1)
    tallies = tallies.at[source_of].add(-passed).at[sink].add(passed)
    members = jnp.searchsorted(jnp.cumsum(tallies), jnp.arange(rows * top), side="right").astype(jnp.int32)
    table = members.reshape(top, rows).T
    table = table[jax.random.permutation(jax.random.fold_in(own, 1), rows)]
    turn = jax.random.randint(jax.random.fold_in(own, 2), (rows, 1), 0, top)
    return jnp.take_along_axis(table, (jnp.arange(top)[None, :] + turn) % top, axis=1)


def load_shares(number_of, total, bound, lean, full):
    loads = [(1 << 20) // math.isqrt(standing ** lean) + 1 for standing in range(1, number_of + 1)]
    largest = bound if full else min(bound, max(-(-total // number_of), total * loads[0] // sum(loads)))
    least = 1 if total - largest >= number_of - 1 else 0
    counts, surplus = [largest] + [least] * (number_of - 1), total - largest - least * (number_of - 1)
    while surplus > 0:
        free = [i for i in range(1, number_of) if counts[i] < largest] or [i for i in range(1, number_of) if counts[i] < bound]
        whole, remaining = sum([loads[i] for i in free]), surplus
        for i in free:
            extra = min(bound - counts[i], max(1, remaining * loads[i] // whole), surplus)
            counts[i] = counts[i] + extra
            surplus = surplus - extra
    return np.array(counts)


def gaussian(own_key, dims, spread, bound, split=(), kind=jnp.bfloat16):
    result = spread * jax.random.normal(own_key, dims, jnp.float32)
    if split:
        result = result * block_scale(own_key, dims, split, -0.22, 0.18)
    return jnp.clip(result, -bound, bound).astype(kind)


def setup_inputs(seed: int = 0, part: int = 0) -> dict:
    arg_keys = jax.random.split(jax.random.key(seed), 6)
    own_keys = jax.random.split(jax.random.fold_in(arg_keys[5], part), 6)
    tokens = gaussian(own_keys[0], (TOKENS, D), 1.0, 6.0, ((0, 64), (1, 4)))
    expert_ids_keys = jax.random.split(jax.random.fold_in(own_keys[1], 1), TOKENS // TOK_DEV)
    expert_ids_turns = jax.random.permutation(jax.random.fold_in(own_keys[1], 3), TOKENS // TOK_DEV)
    expert_ids = jax.vmap(lambda own, number: deal_out(jax.random.fold_in(own_keys[1], 2), own, number, TOK_DEV, EXPERTS, TOP, CAP, 2))(expert_ids_keys, expert_ids_turns).reshape((TOKENS, TOP))
    router_logits = gaussian(own_keys[2], (TOKENS, TOP), 1.5, 6.0, ((0, 64),), jnp.float32)
    up_weight = gaussian(arg_keys[3], (EXPERTS, D, FF), D ** -0.5, 0.09375, ((0, 64), (2, 4)))
    down_weight = gaussian(arg_keys[4], (EXPERTS, FF, D), FF ** -0.5, 0.1875, ((0, 64), (1, 4)))
    return {"tokens": tokens, "expert_ids": expert_ids, "router_logits": router_logits, "up_weight": up_weight, "down_weight": down_weight}


def reference(tokens, expert_ids, router_logits, up_weight, down_weight):
    ids = expert_ids.reshape(N_EXPERT, TOK_DEV, TOP)
    hits = (ids[:, :, :, None] == jnp.arange(EXPERTS, dtype=jnp.int32)[None, None, None, :]).astype(jnp.int32)
    per_token = jnp.sum(hits, axis=2)
    rank = jnp.cumsum(per_token, axis=1) - per_token
    slot = jnp.sum(hits * rank[:, :, None, :], axis=3)
    block = jnp.arange(N_EXPERT, dtype=jnp.int32)[:, None, None]
    row = (block * CAP + slot).astype(jnp.int32)
    token_index = (block * TOK_DEV + jnp.arange(TOK_DEV, dtype=jnp.int32)[None, :, None]) + jnp.zeros_like(ids)
    table = jnp.full((EXPERTS, N_EXPERT * CAP), -1, dtype=jnp.int32)
    table = table.at[ids.reshape(-1), row.reshape(-1)].set(token_index.reshape(-1).astype(jnp.int32))
    quarter = FF // N_TENSOR

    def one_expert(packed):
        index, w_up, w_down = packed
        valid = (index >= 0)[:, None]
        rows = jnp.where(valid, tokens[jnp.maximum(index, 0)], jnp.zeros((), jnp.bfloat16))
        act = jnp.dot(rows, w_up, preferred_element_type=jnp.float32)
        hidden = jax.nn.silu(act).astype(jnp.bfloat16)
        pieces = hidden.reshape(-1, N_TENSOR, quarter).astype(jnp.float32)
        blocks = w_down.reshape(N_TENSOR, quarter, D).astype(jnp.float32)
        parts = jnp.einsum("rjf,jfd->jrd", pieces, blocks)
        parts = parts.astype(jnp.bfloat16).astype(jnp.float32)
        return jnp.sum(parts, axis=0).astype(jnp.bfloat16)

    expert_out = lax.map(one_expert, (table, up_weight, down_weight))
    picked = expert_out[ids.reshape(-1), row.reshape(-1)].astype(jnp.float32).reshape(TOKENS, TOP, D)
    gates = jax.nn.sigmoid(router_logits)
    weight = 2.5 * gates / jnp.sum(gates, axis=1, keepdims=True)
    return jnp.sum(weight[:, :, None] * picked, axis=1).astype(jnp.bfloat16)
```

```python
import jax
import jax.numpy as jnp
from jax import lax
from jax.sharding import Mesh
from jax.sharding import PartitionSpec as P

EXPERT = ("z", "core")
GROUP_EXPERT = ("group", "z", "core")


def shifted(x, axis, by):
    n = lax.axis_size(axis)
    return lax.ppermute(x, axis, [(i, (i + by) % n) for i in range(n)])


def slots_of(expert_ids, experts):
    hits = (expert_ids[:, :, None] == jnp.arange(experts, dtype=jnp.int32)).astype(jnp.int32)
    per_token = jnp.sum(hits, axis=1)
    rank = jnp.cumsum(per_token, axis=0) - per_token
    return jnp.sum(hits * rank[:, None, :], axis=2)


def on_device(tokens, expert_ids, router_logits, up_weight, down_weight):
    tok_rows, width = tokens.shape
    top_count = expert_ids.shape[1]
    chips = lax.axis_size("z")
    cores = lax.axis_size("core")
    experts = chips * cores
    parts = lax.axis_size("tensor")
    capacity = max(2, 3 * tok_rows * top_count // (2 * experts))
    quarter = up_weight.shape[2]
    me_core = lax.axis_index("core")
    me_part = lax.axis_index("tensor")

    up, down = up_weight[0], down_weight[0]
    up_pieces, down_pieces = [], []
    for d in range(parts):
        target = (me_part + d) % parts
        mine = lax.dynamic_slice_in_dim(up, target * width, width, 0)
        up_pieces.append(shifted(mine, "tensor", d) if d else mine)
    for d in range(parts):
        target = (me_part + d) % parts
        mine = lax.dynamic_slice_in_dim(down, target * width, width, 1)
        down_pieces.append(shifted(mine, "tensor", d) if d else mine)

    slot = slots_of(expert_ids, experts)
    gates = jax.nn.sigmoid(router_logits)
    weight = 2.5 * gates / jnp.sum(gates, axis=1, keepdims=True)
    place = (expert_ids * capacity + slot).astype(jnp.float32)
    notes = jnp.concatenate([place, weight], axis=1)
    other_notes = shifted(notes, "core", 1)
    other_tokens = shifted(tokens, "core", 1)
    chip_tokens = jnp.concatenate([tokens, other_tokens], axis=0)
    chip_notes = jnp.concatenate([notes, other_notes], axis=0)
    chip_place = chip_notes[:, :top_count].astype(jnp.int32)
    chip_weight = chip_notes[:, top_count:]
    chip_expert = chip_place // capacity
    block = (jnp.arange(cores * tok_rows, dtype=jnp.int32) // tok_rows)[:, None]
    rows_each = cores * capacity
    position = (chip_expert // cores) * rows_each + block * capacity + chip_place % capacity
    position = jnp.where(chip_expert % cores == me_core, position, -1)
    rows = chips * rows_each
    chosen = position[:, :, None] == jnp.arange(rows, dtype=jnp.int32)

    selector = jnp.any(chosen, axis=1).astype(jnp.bfloat16)
    outgoing = jnp.einsum(
        "tr,td->rd", selector, chip_tokens, preferred_element_type=jnp.float32
    ).astype(jnp.bfloat16)
    arrived = lax.all_to_all(
        outgoing.reshape(chips, rows_each, width), "z", 0, 0, tiled=True
    ).reshape(rows, width)

    act = None
    sums = []
    for d in (2, 1, 3, 0):
        part = jnp.dot(arrived, up_pieces[d], preferred_element_type=jnp.float32)
        if d:
            sums.append(shifted(part.astype(jnp.bfloat16), "tensor", -d))
        else:
            act = part
    for piece in sums:
        act = act + piece.astype(jnp.float32)
    hidden = jax.nn.silu(act).astype(jnp.bfloat16)

    total = None
    for d in (0, 1, 3, 2):
        piece = shifted(hidden, "tensor", d) if d else hidden
        term = jnp.dot(piece, down_pieces[d], preferred_element_type=jnp.float32)
        total = term if total is None else total + term
    returned = lax.all_to_all(
        total.astype(jnp.bfloat16).reshape(chips, rows_each, width), "z", 0, 0, tiled=True
    ).reshape(rows, width)

    mixer = jnp.sum(jnp.where(chosen, chip_weight[:, :, None], 0.0), axis=1)
    high = lax.reduce_precision(mixer, 8, 7)
    low = mixer - high
    mixed = jnp.dot(
        jnp.concatenate([high, low], axis=0).astype(jnp.bfloat16),
        returned,
        preferred_element_type=jnp.float32,
    )
    n = cores * tok_rows
    mixed = mixed[:n] + mixed[n:]
    theirs = shifted(mixed[tok_rows:], "core", 1)
    return (mixed[:tok_rows] + theirs).astype(jnp.bfloat16)


def solution(mesh):
    cores = 2
    chips = mesh.shape["expert"] // cores
    split = Mesh(
        mesh.devices.reshape(mesh.shape["group"], chips, cores, mesh.shape["tensor"]),
        ("group", "z", "core", "tensor"),
    )
    return jax.shard_map(
        on_device,
        mesh=split,
        in_specs=(
            P(GROUP_EXPERT, "tensor"),
            P(GROUP_EXPERT, None),
            P(GROUP_EXPERT, None),
            P(EXPERT, None, "tensor"),
            P(EXPERT, "tensor", None),
        ),
        out_specs=P(GROUP_EXPERT, "tensor"),
        check_vma=False,
    )
```

```python
import jax
import jax.numpy as jnp
from jax import lax
from jax.sharding import Mesh
from jax.sharding import PartitionSpec as P

EXPERT = ("z", "core")
GROUP_EXPERT = ("group", "z", "core")


def shifted(x, axis, by):
    n = lax.axis_size(axis)
    return lax.ppermute(x, axis, [(i, (i + by) % n) for i in range(n)])


def slots_of(expert_ids, experts):
    hits = (expert_ids[:, :, None] == jnp.arange(experts, dtype=jnp.int32)).astype(jnp.int32)
    per_token = jnp.sum(hits, axis=1)
    rank = jnp.cumsum(per_token, axis=0) - per_token
    return jnp.sum(hits * rank[:, None, :], axis=2)


def on_device(tokens, expert_ids, router_logits, up_weight, down_weight):
    tok_rows, width = tokens.shape
    top_count = expert_ids.shape[1]
    chips = lax.axis_size("z")
    cores = lax.axis_size("core")
    experts = chips * cores
    parts = lax.axis_size("tensor")
    capacity = max(2, 3 * tok_rows * top_count // (2 * experts))
    lanes = 256
    me_core = lax.axis_index("core")
    me_part = lax.axis_index("tensor")

    up, down = up_weight[0], down_weight[0]
    up_pieces, down_pieces = [], []
    for d in range(parts):
        target = (me_part + d) % parts
        mine = lax.dynamic_slice_in_dim(up, target * width, width, 0)
        up_pieces.append(shifted(mine, "tensor", d) if d else mine)
    for d in range(parts):
        target = (me_part + d) % parts
        mine = lax.dynamic_slice_in_dim(down, target * width, width, 1)
        down_pieces.append(shifted(mine, "tensor", d) if d else mine)

    slot = slots_of(expert_ids, experts)
    gates = jax.nn.sigmoid(router_logits)
    weight = 2.5 * gates / jnp.sum(gates, axis=1, keepdims=True)
    place = (expert_ids * capacity + slot).astype(jnp.float32)
    notes = jnp.concatenate([place, weight], axis=1)
    other_notes = shifted(notes, "core", 1)
    other_tokens = shifted(tokens, "core", 1)
    chip_tokens = jnp.concatenate([tokens, other_tokens], axis=0)
    chip_notes = jnp.concatenate([notes, other_notes], axis=0)
    chip_place = chip_notes[:, :top_count].astype(jnp.int32)
    chip_weight = chip_notes[:, top_count:]
    chip_expert = chip_place // capacity
    block = (jnp.arange(cores * tok_rows, dtype=jnp.int32) // tok_rows)[:, None]
    tokens_here = cores * tok_rows
    rows_each = cores * capacity
    folds = width // lanes
    position = (chip_expert // cores) * (folds * rows_each) + block * capacity + chip_place % capacity
    position = jnp.where(chip_expert % cores == me_core, position, -folds * rows_each)
    rows = chips * rows_each
    fold = jnp.arange(folds, dtype=jnp.int32)[:, None, None]
    position = (position[None] + fold * rows_each).reshape(folds * tokens_here, top_count)
    chosen = position[:, :, None] == jnp.arange(folds * rows, dtype=jnp.int32)

    selector = jnp.any(chosen, axis=1).astype(jnp.bfloat16)
    folded = jnp.concatenate(
        [chip_tokens[:, f * lanes : (f + 1) * lanes] for f in range(folds)], axis=0
    )
    outgoing = jnp.einsum(
        "tr,td->rd", selector, folded, preferred_element_type=jnp.float32
    ).astype(jnp.bfloat16)
    arrived = lax.all_to_all(
        outgoing.reshape(chips, folds * rows_each, lanes), "z", 0, 0, tiled=True
    )
    arrived = arrived.reshape(chips, folds, rows_each, lanes)
    arrived = jnp.moveaxis(arrived, 1, 2).reshape(rows, width)

    act = None
    sums = []
    for d in (2, 1, 3, 0):
        part = jnp.dot(arrived, up_pieces[d], preferred_element_type=jnp.float32)
        if d:
            sums.append(shifted(part.astype(jnp.bfloat16), "tensor", -d))
        else:
            act = part
    for piece in sums:
        act = act + piece.astype(jnp.float32)
    hidden = jax.nn.silu(act).astype(jnp.bfloat16)

    total = None
    for d in (0, 1, 3, 2):
        piece = shifted(hidden, "tensor", d) if d else hidden
        term = jnp.dot(piece, down_pieces[d], preferred_element_type=jnp.float32)
        total = term if total is None else total + term
    going = total.astype(jnp.bfloat16).reshape(chips, rows_each, folds, lanes)
    going = jnp.moveaxis(going, 2, 1).reshape(chips, folds * rows_each, lanes)
    returned = lax.all_to_all(going, "z", 0, 0, tiled=True).reshape(folds * rows, lanes)

    weights = jnp.concatenate([chip_weight] * folds, axis=0)
    mixer = jnp.sum(jnp.where(chosen, weights[:, :, None], 0.0), axis=1)
    high = lax.reduce_precision(mixer, 8, 7)
    low = mixer - high
    n = folds * tokens_here
    mixed = jnp.dot(
        jnp.concatenate([high, low], axis=0).astype(jnp.bfloat16),
        returned,
        preferred_element_type=jnp.float32,
    )
    mixed = mixed[:n] + mixed[n:]
    mixed = jnp.concatenate(
        [mixed[f * tokens_here : (f + 1) * tokens_here] for f in range(folds)], axis=1
    )
    theirs = shifted(mixed[tok_rows:], "core", 1)
    return (mixed[:tok_rows] + theirs).astype(jnp.bfloat16)


def solution(mesh):
    cores = 2
    chips = mesh.shape["expert"] // cores
    split = Mesh(
        mesh.devices.reshape(mesh.shape["group"], chips, cores, mesh.shape["tensor"]),
        ("group", "z", "core", "tensor"),
    )
    return jax.shard_map(
        on_device,
        mesh=split,
        in_specs=(
            P(GROUP_EXPERT, "tensor"),
            P(GROUP_EXPERT, None),
            P(GROUP_EXPERT, None),
            P(EXPERT, None, "tensor"),
            P(EXPERT, "tensor", None),
        ),
        out_specs=P(GROUP_EXPERT, "tensor"),
        check_vma=False,
    )
```

```python
import jax
import jax.numpy as jnp
from jax import lax
from jax.sharding import Mesh
from jax.sharding import PartitionSpec as P

EXPERT = ("z", "core")
GROUP_EXPERT = ("group", "z", "core")
STRIDE = 8
NEAR = STRIDE // 2


def shifted(x, axis, by):
    n = lax.axis_size(axis)
    return lax.ppermute(x, axis, [(i, (i + by) % n) for i in range(n)])


def slots_of(expert_ids, experts):
    hits = (expert_ids[:, :, None] == jnp.arange(experts, dtype=jnp.int32)).astype(jnp.int32)
    per_token = jnp.sum(hits, axis=1)
    rank = jnp.cumsum(per_token, axis=0) - per_token
    return jnp.sum(hits * rank[:, None, :], axis=2)


def layer(tokens, expert_ids, router_logits, up_weight, down_weight):
    tok_rows, width = tokens.shape
    top_count = expert_ids.shape[1]
    chips = lax.axis_size("z")
    cores = lax.axis_size("core")
    experts = chips * cores
    parts = lax.axis_size("tensor")
    capacity = max(2, 3 * tok_rows * top_count // (2 * experts))
    me_chip = lax.axis_index("z")
    me_core = lax.axis_index("core")
    me_part = lax.axis_index("tensor")
    half = tok_rows // 2

    behind = shifted(tokens, "z", STRIDE)
    ahead = shifted(tokens, "z", -STRIDE)
    slot = slots_of(expert_ids, experts)
    place = (expert_ids * capacity + slot).astype(jnp.float32)
    notes = jnp.concatenate([place, router_logits], axis=1)
    notes_behind = shifted(notes, "z", STRIDE)
    notes_ahead = shifted(notes, "z", -STRIDE)
    opposite_top = shifted(behind[:half], "z", STRIDE)
    opposite_bottom = shifted(ahead[half:], "z", -STRIDE)
    notes_opposite = shifted(notes_behind, "z", STRIDE)
    blocks = jnp.concatenate([tokens, behind, ahead, opposite_top, opposite_bottom], axis=0)
    notes = jnp.concatenate([notes, notes_behind, notes_ahead, notes_opposite], axis=0)

    each = (chips // STRIDE) * capacity
    near = tuple(range(1 - NEAR, NEAR))
    pairs = len(near)
    rows = (pairs + 1) * cores * each
    place = notes[:, :top_count].astype(jnp.int32)
    expert = place // capacity
    offset = (expert // cores - me_chip + chips + NEAR) % chips - NEAR
    across = jnp.where(expert % cores == me_core, 0, 1)
    block = (jnp.arange(place.shape[0], dtype=jnp.int32) // tok_rows)[:, None]
    row = ((offset + NEAR - 1) * cores + across) * each
    row = jnp.where((offset == NEAR) & (across == 0), pairs * cores * each, row)
    row = jnp.where((offset == -NEAR) & (across == 1), (pairs * cores + 1) * each, row)
    kept = (jnp.abs(offset) < NEAR) | (offset == NEAR * (1 - 2 * across))
    row = jnp.where(kept, row + block * capacity + place % capacity, -1)
    chosen = row[:, :, None] == jnp.arange(rows, dtype=jnp.int32)
    selector = jnp.any(chosen, axis=1).astype(jnp.bfloat16)
    outgoing = jnp.einsum(
        "tr,td->rd", selector, blocks, preferred_element_type=jnp.float32
    ).astype(jnp.bfloat16)

    hops = [(o, (o + NEAR - 1) * cores * each, cores * each) for o in near]
    hops += [(NEAR, pairs * cores * each, each), (-NEAR, (pairs * cores + 1) * each, each)]
    arrived = {}
    for o, start, count in sorted(hops, key=lambda h: -abs(h[0])):
        piece = outgoing[start : start + count]
        arrived[o] = shifted(piece, "z", o) if o else piece
    arrived = lax.optimization_barrier(arrived)
    mine = jnp.concatenate([arrived[o][:each] for o in near] + [arrived[NEAR]], axis=0)
    theirs = jnp.concatenate([arrived[o][each:] for o in near] + [arrived[-NEAR]], axis=0)
    rows_in = jnp.concatenate([mine, shifted(theirs, "core", 1)], axis=0)

    up, down = up_weight[0], down_weight[0]
    up_pieces, down_pieces = [], []
    for d in range(parts):
        target = (me_part + d) % parts
        piece = lax.dynamic_slice_in_dim(up, target * width, width, 0)
        up_pieces.append(shifted(piece, "tensor", d) if d else piece)
    for d in range(parts):
        target = (me_part + d) % parts
        piece = lax.dynamic_slice_in_dim(down, target * width, width, 1)
        down_pieces.append(shifted(piece, "tensor", d) if d else piece)

    act = None
    sums = []
    for d in (2, 1, 3, 0):
        part = jnp.dot(rows_in, up_pieces[d], preferred_element_type=jnp.float32)
        if d:
            sums.append(shifted(part.astype(jnp.bfloat16), "tensor", -d))
        else:
            act = part
    for piece in sums:
        act = act + piece.astype(jnp.float32)
    hidden = jax.nn.silu(act).astype(jnp.bfloat16)
    total = None
    for d in (0, 1, 3, 2):
        piece = shifted(hidden, "tensor", d) if d else hidden
        term = jnp.dot(piece, down_pieces[d], preferred_element_type=jnp.float32)
        total = term if total is None else total + term
    out = total.astype(jnp.bfloat16)

    mine = out[: rows // 2]
    theirs = shifted(out[rows // 2 :], "core", 1)
    back = {}
    for o in sorted(near, key=lambda h: -abs(h)):
        i = (o + NEAR - 1) * each
        piece = jnp.concatenate([mine[i : i + each], theirs[i : i + each]], axis=0)
        back[o] = shifted(piece, "z", -o) if o else piece
    back[NEAR] = shifted(mine[pairs * each :], "z", -NEAR)
    back[-NEAR] = shifted(theirs[pairs * each :], "z", NEAR)
    back = lax.optimization_barrier(back)
    returned = jnp.concatenate([back[h[0]] for h in hops], axis=0)

    gates = jax.nn.sigmoid(notes[:, top_count:])
    weight = 2.5 * gates / jnp.sum(gates, axis=1, keepdims=True)
    mixer = jnp.sum(jnp.where(chosen, weight[:, :, None], 0.0), axis=1)
    high = lax.reduce_precision(mixer, 8, 7)
    low = mixer - high
    n = mixer.shape[0]
    both = jnp.dot(
        jnp.concatenate([high, low], axis=0).astype(jnp.bfloat16),
        returned,
        preferred_element_type=jnp.float32,
    )
    sums = (both[:n] + both[n:]).reshape(-1, tok_rows, width)
    own, behind, ahead, opposite = sums[0], sums[1], sums[2], sums[3]

    opposite = opposite.astype(jnp.bfloat16)
    top = shifted(opposite[:half], "z", STRIDE).astype(jnp.float32)
    bottom = shifted(opposite[half:], "z", -STRIDE).astype(jnp.float32)
    ahead = jnp.concatenate([ahead[:half] + top, ahead[half:]], axis=0).astype(jnp.bfloat16)
    behind = jnp.concatenate([behind[:half], behind[half:] + bottom], axis=0).astype(jnp.bfloat16)
    from_behind = shifted(ahead, "z", STRIDE)
    from_ahead = shifted(behind, "z", -STRIDE)
    own = own + from_behind.astype(jnp.float32) + from_ahead.astype(jnp.float32)
    return own.astype(jnp.bfloat16)


def solution(mesh):
    cores = 2
    chips = mesh.shape["expert"] // cores
    split = Mesh(
        mesh.devices.reshape(mesh.shape["group"], chips, cores, mesh.shape["tensor"]),
        ("group", "z", "core", "tensor"),
    )
    return jax.shard_map(
        layer,
        mesh=split,
        in_specs=(
            P(GROUP_EXPERT, "tensor"),
            P(GROUP_EXPERT, None),
            P(GROUP_EXPERT, None),
            P(EXPERT, None, "tensor"),
            P(EXPERT, "tensor", None),
        ),
        out_specs=P(GROUP_EXPERT, "tensor"),
        check_vma=False,
    )
```

```python
import jax
import jax.numpy as jnp
from jax import lax
from jax.sharding import Mesh
from jax.sharding import PartitionSpec as P

EXPERT = ("z", "core")
GROUP_EXPERT = ("group", "z", "core")
LANES = 256


def shifted(x, axis, by):
    n = lax.axis_size(axis)
    return lax.ppermute(x, axis, [(i, (i + by) % n) for i in range(n)])


def on_device(tokens, expert_ids, router_logits, up_weight, down_weight):
    tok_rows, width = tokens.shape
    top_count = expert_ids.shape[1]
    experts = lax.axis_size("z") * lax.axis_size("core")
    parts = lax.axis_size("tensor")
    capacity = max(2, 3 * tok_rows * top_count // (2 * experts))
    folds = width // LANES
    piece_rows = folds * capacity
    rows = experts * piece_rows
    me_part = lax.axis_index("tensor")

    r = jnp.arange(rows, dtype=jnp.int32)
    of_expert = (r[None, :] // piece_rows == jnp.arange(experts, dtype=jnp.int32)[:, None]).astype(
        jnp.bfloat16
    )
    fold_of = r % piece_rows // capacity
    slot_of = (r % capacity).astype(jnp.float32)

    def spread(by_expert):
        return jnp.dot(by_expert, of_expert, preferred_element_type=jnp.float32)

    hits = expert_ids[:, :, None] == jnp.arange(experts, dtype=jnp.int32)
    named = jnp.any(hits, axis=1)
    count = named.astype(jnp.int32)
    rank = jnp.cumsum(count, axis=0) - count
    rank = jnp.where(named, rank, -1).astype(jnp.bfloat16)
    taken = spread(rank) == slot_of
    mask = jnp.concatenate([taken & (fold_of == f) for f in range(folds)], axis=0)

    folded = jnp.concatenate(
        [tokens[:, f * LANES : (f + 1) * LANES] for f in range(folds)], axis=0
    )
    outgoing = jnp.einsum(
        "tr,td->rd", mask.astype(jnp.bfloat16), folded, preferred_element_type=jnp.float32
    ).astype(jnp.bfloat16)
    arrived = lax.all_to_all(
        outgoing.reshape(experts, piece_rows, LANES), EXPERT, 0, 0, tiled=True
    )
    late = lax.optimization_barrier((router_logits, hits, mask, arrived))
    arrived = late[-1].reshape(experts, folds, capacity, LANES)
    arrived = jnp.moveaxis(arrived, 1, 2).reshape(experts * capacity, width)

    up, down = up_weight[0], down_weight[0]
    up_all = jnp.zeros((parts, width, up.shape[1]), up.dtype)
    down_all = jnp.zeros((parts, down.shape[0], width), down.dtype)
    for d in range(parts):
        target, source = (me_part + d) % parts, (me_part - d) % parts
        piece = lax.dynamic_slice_in_dim(up, target * width, width, 0)
        piece = shifted(piece, "tensor", d) if d else piece
        up_all = lax.dynamic_update_slice_in_dim(up_all, piece[None], source, 0)
    for d in range(parts):
        target, source = (me_part + d) % parts, (me_part - d) % parts
        piece = lax.dynamic_slice_in_dim(down, target * width, width, 1)
        piece = shifted(piece, "tensor", d) if d else piece
        down_all = lax.dynamic_update_slice_in_dim(down_all, piece[None], source, 0)

    sums = jnp.stack(
        [
            jnp.dot(arrived, up_all[p], preferred_element_type=jnp.float32).astype(jnp.bfloat16)
            for p in range(parts)
        ]
    )
    sums = lax.all_to_all(sums, "tensor", 0, 0, tiled=True)
    act = jnp.sum(sums.astype(jnp.float32), axis=0)
    hidden = jax.nn.silu(act).astype(jnp.bfloat16)
    hidden = lax.all_gather(hidden, "tensor", axis=1, tiled=True)
    out = jnp.dot(
        hidden, down_all.reshape(-1, width), preferred_element_type=jnp.float32
    ).astype(jnp.bfloat16)

    going = jnp.moveaxis(out.reshape(experts, capacity, folds, LANES), 2, 1)
    returned = lax.all_to_all(
        going.reshape(experts, piece_rows, LANES), EXPERT, 0, 0, tiled=True
    ).reshape(rows, LANES)

    router_logits, hits, mask, _ = late
    gates = jax.nn.sigmoid(router_logits)
    weight = 2.5 * gates / jnp.sum(gates, axis=1, keepdims=True)
    weight = jnp.sum(jnp.where(hits, weight[:, :, None], 0.0), axis=1)
    high = lax.reduce_precision(weight, 8, 7)
    low = weight - high
    mixer = spread(jnp.concatenate([high, low], axis=0).astype(jnp.bfloat16))
    mixer = mixer.astype(jnp.bfloat16).reshape(2, tok_rows, rows)
    none = jnp.zeros((), jnp.bfloat16)
    n = folds * tok_rows
    mixer = jnp.concatenate(
        [
            jnp.where(mask[f * tok_rows : (f + 1) * tok_rows], mixer[part], none)
            for part in range(2)
            for f in range(folds)
        ],
        axis=0,
    )
    mixed = jnp.dot(mixer, returned, preferred_element_type=jnp.float32)
    mixed = mixed[:n] + mixed[n:]
    mixed = jnp.concatenate(
        [mixed[f * tok_rows : (f + 1) * tok_rows] for f in range(folds)], axis=1
    )
    return mixed.astype(jnp.bfloat16)


def solution(mesh):
    cores = 2
    chips = mesh.shape["expert"] // cores
    split = Mesh(
        mesh.devices.reshape(mesh.shape["group"], chips, cores, mesh.shape["tensor"]),
        ("group", "z", "core", "tensor"),
    )
    return jax.shard_map(
        on_device,
        mesh=split,
        in_specs=(
            P(GROUP_EXPERT, "tensor"),
            P(GROUP_EXPERT, None),
            P(GROUP_EXPERT, None),
            P(EXPERT, None, "tensor"),
            P(EXPERT, "tensor", None),
        ),
        out_specs=P(GROUP_EXPERT, "tensor"),
        check_vma=False,
    )
```
